32 devices in a mesh: members: 2 (over x), zonal: 8 (over z, y), merid: 2 (over core).
Axes of the slice: x: 2, y: 2, z: 4, core: 2. Of those that a mesh axis runs over, the one named last changes fastest.
Arguments:
- height: float32 [256, 1024], P(('members', 'zonal'), 'merid'), parts along dimension 0, may hold values from -6 to 6
- transport_u: float32 [256, 1024], P(('members', 'zonal'), 'merid'), parts along dimension 0, may hold values from -4 to 4
- transport_v: float32 [256, 1024], P(('members', 'zonal'), 'merid'), parts along dimension 0, may hold values from -4 to 4
- thickness: float32 [14, 256, 1024], P(None, ('members', 'zonal'), 'merid'), parts along dimension 1, may hold values from 0.5 to 2
- velocity_u: float32 [14, 256, 1024], P(None, ('members', 'zonal'), 'merid'), parts along dimension 1, may hold values from -3 to 3
- velocity_v: float32 [14, 256, 1024], P(None, ('members', 'zonal'), 'merid'), parts along dimension 1, may hold values from -3 to 3
- sea_faces: int32 [2, 128, 1024], P(None, 'zonal', 'merid'), may hold values 0 or 1
- wind_seeds: int32 [8, 2], P('members'), parts along dimension 0, may hold values from 1 to 96
- wind_scale: float32 [8], P('members'), parts along dimension 0, may hold values from 0.5 to 2
- wind_base: float32 [2, 128, 1024], P(None, 'zonal', 'merid'), may hold values from -6 to 6
Outputs:
- final_height: float32 [256, 1024], P(('members', 'zonal'), 'merid'), parts along dimension 0
- final_transport_u: float32 [256, 1024], P(('members', 'zonal'), 'merid'), parts along dimension 0
- final_transport_v: float32 [256, 1024], P(('members', 'zonal'), 'merid'), parts along dimension 0
- final_thickness: float32 [14, 256, 1024], P(None, ('members', 'zonal'), 'merid'), parts along dimension 1
- final_velocity_u: float32 [14, 256, 1024], P(None, ('members', 'zonal'), 'merid'), parts along dimension 1
- final_velocity_v: float32 [14, 256, 1024], P(None, ('members', 'zonal'), 'merid'), parts along dimension 1
The draws below stay inside these ranges and needn't reach their ends.
There are 2 independent parts, one for each index of `members`. The reference program is written for one: setup_inputs(seed, part) draws one part's arguments, and reference() takes and returns one part's arrays. A program takes and returns all parts, laid end to end along the dimension named above; an argument that names none is the same for every part. Nothing has to cross between parts.
All inputs are finite; a program needn't handle non-finite values. No bound on the sum of `sea_faces` on one device may be relied on, other than what follows from the above.
Results may differ from the reference program's by a relative error of at most 0.0001.
Values sent between devices are 32-bit elements; how exact they have to be, the bound alone decides.
No kernel may reach another device: no remote copies, remote signals or barrier semaphores. Data moves between devices by JAX's collectives and lax.ppermute only.
A program may use at most 64 MiB of HBM per device.

```python
import math
import jax
import jax.numpy as jnp

LAYERS = 14
NSUB = 6
STEPS = 2
MODES = 4
NX = 128
NY = 1024


def plant(result, stream_key, least, top_value):
    spot = [jax.random.randint(jax.random.fold_in(stream_key, axis), (), 0, length) for axis, length in enumerate(result.shape)]
    widest = result.shape.index(max(result.shape))
    beside = spot[:widest] + [(spot[widest] + 1) % result.shape[widest]] + spot[widest + 1:]
    return result.at[tuple(spot)].set(least).at[tuple(beside)].set(top_value)


def block_scale(own_key, extent, shards, least, largest):
    def one(dim, blocks):
        heights = jax.random.uniform(jax.random.fold_in(jax.random.fold_in(own_key, 6), dim), (blocks,), jnp.float32, least / len(shards), largest / len(shards))
        return jnp.repeat(jnp.exp(heights), extent[dim] // blocks).reshape((-1,) + (1,) * (len(extent) - dim - 1))

    gain = one(*shards[0])
    for cut in shards[1:]:
        gain = gain * one(*cut)
    return gain


def noise(rng, shape, deviation, limit, split=(), kind=jnp.bfloat16):
    gain = block_scale(rng, shape, split, -0.22, 0.18) if split else 1.0
    entries = jax.random.normal(rng, shape, jnp.float32) * deviation * gain
    return jnp.minimum(jnp.maximum(entries, -limit), limit).astype(kind)


def setup_inputs(seed: int = 0, part: int = 0) -> dict:
    splits = jax.random.split(jax.random.key(seed), 11)
    part_splits = jax.random.split(jax.random.fold_in(splits[10], part), 11)
    return {
        "height": noise(part_splits[0], (NX, NY), 1.0, 6.0, ((0, 8), (1, 2)), jnp.float32),
        "transport_u": noise(part_splits[1], (NX, NY), 0.5, 4.0, ((0, 8), (1, 2)), jnp.float32),
        "transport_v": noise(part_splits[2], (NX, NY), 0.5, 4.0, ((0, 8), (1, 2)), jnp.float32),
        "thickness": jnp.clip(jnp.exp(math.log(2.0) - 1.3862944 * jax.random.uniform(part_splits[3], (LAYERS, NX, NY), jnp.float32) ** block_scale(part_splits[3], (LAYERS, NX, NY), ((1, 8), (2, 2)), -0.2, 0.2)), 0.5, 2.0),
        "velocity_u": noise(part_splits[4], (LAYERS, NX, NY), 0.5, 3.0, ((1, 8), (2, 2)), jnp.float32),
        "velocity_v": noise(part_splits[5], (LAYERS, NX, NY), 0.5, 3.0, ((1, 8), (2, 2)), jnp.float32),
        "sea_faces": plant((jax.random.randint(splits[6], (2, NX, NY), 0, 8) < 7).astype(jnp.int32), jax.random.fold_in(splits[6], 1), 0, 1),
        "wind_seeds": plant(jax.random.randint(part_splits[7], (MODES, 2), 1, 97), jax.random.fold_in(part_splits[7], 1), 1, 96).astype(jnp.int32),
        "wind_scale": jnp.clip(jnp.exp(jax.random.uniform(part_splits[8], (MODES,), jnp.float32, math.log(0.5), math.log(2.0))), 0.5, 2.0),
        "wind_base": noise(splits[9], (2, NX, NY), 1.0, 6.0, ((1, 8), (2, 2)), jnp.float32),
    }


WAVE_LIMIT = 0.225
STRESS_SCALE = 0.1
FLUX_STEP = 0.05
PRESS_COEF = 0.05


def east(field):
    return jnp.roll(field, -1, axis=-2)


def west(field):
    return jnp.roll(field, 1, axis=-2)


def north(field):
    folded = jnp.flip(field[..., -1], axis=-1)
    return jnp.concatenate([field[..., 1:], folded[..., None]], axis=-1)


def south(field):
    return jnp.concatenate([jnp.zeros_like(field[..., :1]), field[..., :-1]], axis=-1)


def reference(height, transport_u, transport_v, thickness, velocity_u, velocity_v, sea_faces, wind_seeds, wind_scale, wind_base):
    total_x = height.shape[0]
    total_y = height.shape[1]
    mask_u = sea_faces[0].astype(jnp.float32)
    mask_v = sea_faces[1].astype(jnp.float32)
    columns = jnp.arange(total_x, dtype=jnp.int32)
    rows_idx = jnp.arange(total_y, dtype=jnp.int32)
    wave_x = wind_seeds[:, 0].astype(jnp.int32)
    wave_y = wind_seeds[:, 1].astype(jnp.int32)
    phase = ((wave_x[:, None, None] * columns[None, :, None]) % total_x).astype(jnp.float32) / total_x
    phase = phase + ((wave_y[:, None, None] * rows_idx[None, None, :]) % total_y).astype(jnp.float32) / total_y
    angle = (2.0 * math.pi) * phase
    amplitude = wind_scale[:, None, None]
    stress_x = STRESS_SCALE * (wind_base[0] + jnp.sum(amplitude * jnp.cos(angle), axis=0))
    stress_y = STRESS_SCALE * (wind_base[1] + jnp.sum(amplitude * jnp.sin(angle), axis=0))
    layers = thickness.shape[0]
    wave = (WAVE_LIMIT / layers) * jnp.sum(thickness, axis=0)
    depth_u = jnp.sum((thickness + east(thickness)) * 0.5, axis=0)
    depth_v = jnp.sum((thickness + north(thickness)) * 0.5, axis=0)
    surface, flow_u, flow_v = height, transport_u, transport_v
    thick, speed_u, speed_v = thickness, velocity_u, velocity_v
    for outer in range(STEPS):
        mean_u = jnp.zeros_like(surface)
        mean_v = jnp.zeros_like(surface)
        for inner in range(NSUB):
            surface = surface - (flow_u - west(flow_u) + flow_v - south(flow_v))
            flow_u = mask_u * (flow_u - wave * (east(surface) - surface) + stress_x)
            flow_v = mask_v * (flow_v - wave * (north(surface) - surface) + stress_y)
            mean_u = mean_u + flow_u
            mean_v = mean_v + flow_v
        mean_u = mean_u / NSUB
        mean_v = mean_v / NSUB
        thick_u = (thick + east(thick)) * 0.5
        thick_v = (thick + north(thick)) * 0.5
        flux_u = speed_u * thick_u
        flux_v = speed_v * thick_v
        pressure = jnp.cumsum(thick, axis=0)
        trial_u = speed_u - PRESS_COEF * (east(pressure) - pressure)
        trial_v = speed_v - PRESS_COEF * (north(pressure) - pressure)
        speed_u = mask_u * (trial_u + (mean_u - jnp.sum(thick_u * trial_u, axis=0)) / depth_u)
        speed_v = mask_v * (trial_v + (mean_v - jnp.sum(thick_v * trial_v, axis=0)) / depth_v)
        thick = thick - FLUX_STEP * (flux_u - west(flux_u) + flux_v - south(flux_v))
    return surface, flow_u, flow_v, thick, speed_u, speed_v
```

```python
import math

import jax
import jax.numpy as jnp
from jax import lax
from jax.experimental import pallas as pl
from jax.experimental.pallas import tpu as pltpu
from jax.sharding import PartitionSpec as P

NSUB = 6
STEPS = 2
WAVE_LIMIT = 0.225
STRESS_SCALE = 0.1
FLUX_STEP = 0.05
PRESS_COEF = 0.05

FIELDS = 8
HALO = NSUB * STEPS
SLOT = 16
LANES = 128
EDGE = 8

VMEM = pl.BlockSpec(memory_space=pltpu.VMEM)
SMEM = pl.BlockSpec(memory_space=pltpu.SMEM)


def whole_mod(product, total):
    rest = product - jnp.floor(product * (1.0 / total)) * total
    rest = jnp.where(rest < 0.0, rest + total, rest)
    return jnp.where(rest >= total, rest - total, rest)


def east_rows(layers):
    return FIELDS * HALO + 4 * layers


def west_rows(layers):
    return FIELDS * HALO + 5 * layers


def prepare_kernel(total_x, total_y, place, seeds, scale, eta, bu, bv, thick, vu, vv, faces, base, fields, to_west, to_east):
    layers, rows, cols = thick.shape
    modes = scale.shape[0]
    f32 = jnp.float32

    lane = lax.broadcasted_iota(jnp.int32, (rows, LANES), 1)
    sub = lax.broadcasted_iota(jnp.int32, (8, cols), 0)
    wave_x = jnp.zeros((rows, LANES), f32)
    wave_y = jnp.zeros((8, cols), f32)
    for m in range(modes):
        wave_x = jnp.where(lane == m, seeds[m, 0].astype(f32), wave_x)
        wave_y = jnp.where(sub == m, seeds[m, 1].astype(f32), wave_y)
    col = (lax.broadcasted_iota(jnp.int32, (rows, LANES), 0) + place[0] * rows).astype(f32)
    row = (lax.broadcasted_iota(jnp.int32, (8, cols), 1) + place[1] * cols).astype(f32)
    angle_x = whole_mod(wave_x * col, total_x) * (2.0 * math.pi / total_x)
    angle_y = whole_mod(wave_y * row, total_y) * (2.0 * math.pi / total_y)
    cos_x, sin_x = jnp.cos(angle_x), jnp.sin(angle_x)
    cos_y, sin_y = jnp.cos(angle_y), jnp.sin(angle_y)
    sum_cos = base[0]
    sum_sin = base[1]
    for m in range(modes):
        amp = scale[m]
        ca = cos_x[:, m : m + 1] * amp
        sa = sin_x[:, m : m + 1] * amp
        cb = cos_y[m : m + 1, :]
        sb = sin_y[m : m + 1, :]
        sum_cos = sum_cos + (ca * cb - sa * sb)
        sum_sin = sum_sin + (sa * cb + ca * sb)
    fields[0] = eta[...]
    fields[1] = bu[...]
    fields[2] = bv[...]
    total = thick[0]
    for k in range(1, layers):
        total = total + thick[k]
    fields[3] = total
    fields[4] = faces[0].astype(f32)
    fields[5] = faces[1].astype(f32)
    fields[6] = STRESS_SCALE * sum_cos
    fields[7] = STRESS_SCALE * sum_sin
    for f in range(FIELDS):
        value = fields[f]
        to_west[f * HALO : (f + 1) * HALO, :] = value[:HALO]
        to_east[f * HALO : (f + 1) * HALO, :] = value[rows - HALO :]
    at = FIELDS * HALO
    for k in range(layers):
        to_west[at + 2 * k : at + 2 * k + 2, :] = thick[k, 0:2, :]
        to_east[at + 2 * k : at + 2 * k + 2, :] = thick[k, rows - 2 : rows, :]
        to_west[at + 2 * layers + k : at + 2 * layers + k + 1, :] = vu[k, 0:1, :]
        to_west[at + 3 * layers + k : at + 3 * layers + k + 1, :] = vv[k, 0:1, :]
        to_east[at + 2 * layers + 2 * k : at + 2 * layers + 2 * k + 2, :] = vu[k, rows - 2 : rows, :]
        to_east[at + 4 * layers + k : at + 4 * layers + k + 1, :] = vv[k, rows - 1 : rows, :]


def fill_fields(target, f, fields, east, west, rows):
    cols = fields.shape[-1]
    target[f, 0:rows, 0:cols] = fields[f]
    target[f, rows : rows + HALO, 0:cols] = east[f * HALO : (f + 1) * HALO, :]
    target[f, rows + HALO : rows + 2 * HALO, 0:cols] = west[f * HALO : (f + 1) * HALO, :]


def fill_layers(target, k, layers, thick, vu, vv, east, west, rows):
    cols = thick.shape[-1]
    at = FIELDS * HALO
    e, w = rows, rows + EDGE
    zero = jnp.zeros((EDGE, cols), jnp.float32)
    for s, own in enumerate((thick, vu, vv)):
        target[s * layers + k, 0:rows, 0:cols] = own[k]
        target[s * layers + k, rows : rows + EDGE, 0:cols] = zero
    target[k, e : e + 2, 0:cols] = east[at + 2 * k : at + 2 * k + 2, :]
    target[k, w - 2 : w, 0:cols] = west[at + 2 * k : at + 2 * k + 2, :]
    target[layers + k, e : e + 1, 0:cols] = east[at + 2 * layers + k : at + 2 * layers + k + 1, :]
    target[layers + k, w - 2 : w, 0:cols] = west[at + 2 * layers + 2 * k : at + 2 * layers + 2 * k + 2, :]
    target[2 * layers + k, e : e + 1, 0:cols] = east[at + 3 * layers + k : at + 3 * layers + k + 1, :]
    target[2 * layers + k, w - 1 : w, 0:cols] = west[at + 4 * layers + k : at + 4 * layers + k + 1, :]


def flipped(pack, rows, group):
    size = pack.shape[0]
    q = lax.broadcasted_iota(jnp.int32, (size, size), 0)
    p = lax.broadcasted_iota(jnp.int32, (size, size), 1)
    source = rows - 1 - q
    source = jnp.where(source < 0, source + size, source)
    flip_rows = (p == source).astype(jnp.float32)
    a = lax.broadcasted_iota(jnp.int32, (LANES, LANES), 0)
    b = lax.broadcasted_iota(jnp.int32, (LANES, LANES), 1)
    inner = jnp.bitwise_and(b, group - 1)
    flip_lanes = (a == b - inner + (group - 1 - inner)).astype(jnp.float32)
    half = jnp.dot(flip_rows, pack, precision=lax.Precision.HIGHEST, preferred_element_type=jnp.float32)
    return jnp.dot(half, flip_lanes, precision=lax.Precision.HIGHEST, preferred_element_type=jnp.float32)


def pack_kernel(
    place,
    fields_a, thick_a, vu_a, vv_a, east_a, west_a,
    fields_b, thick_b, vu_b, vv_b, east_b, west_b,
    low, high, fold, wide, deep,
):
    layers, rows, _ = thick_a.shape
    tall = rows + 2 * HALO
    short = rows + EDGE
    lane_f = lax.broadcasted_iota(jnp.int32, (tall, LANES), 1)
    lane_l = lax.broadcasted_iota(jnp.int32, (short, LANES), 1)
    sides = (
        (low, 0, SLOT, fields_a, thick_a, vu_a, vv_a, east_a, west_a),
        (high, LANES - SLOT, LANES - 2, fields_b, thick_b, vu_b, vv_b, east_b, west_b),
    )
    for out, start, _, fields, thick, vu, vv, east, west in sides:
        first = 0 if start == 0 else LANES - 2
        acc = jnp.zeros((tall, LANES), jnp.float32)
        for f in range(FIELDS):
            fill_fields(wide, f, fields, east, west, rows)
            moved = pltpu.roll(wide[f], (f * SLOT - start) % LANES, 1)
            acc = jnp.where(lane_f // SLOT == f, moved, acc)
        out[0:tall, :] = acc
        acc_l = jnp.zeros((short, LANES), jnp.float32)
        for k in range(layers):
            fill_layers(deep, k, layers, thick, vu, vv, east, west, rows)
        for k in range(3 * layers):
            moved = pltpu.roll(deep[k], (2 * k - first) % LANES, 1)
            acc_l = jnp.where(lane_l // 2 == k, moved, acc_l)
        out[tall : tall + short, :] = acc_l
        if start != 0:
            fold[0:tall, :] = flipped(acc, rows, SLOT)
            fold[tall : tall + short, :] = flipped(acc_l, rows, 2)


def make_neighbours(ghost, cols):
    def east(a):
        n = a.shape[0]
        g = ghost[n]
        plus = pltpu.roll(a, n - 1, 0)
        return jnp.concatenate(
            [plus[:, :cols], jnp.where(g, pltpu.roll(a[:, cols:], 1, 0), plus[:, cols:])], axis=1
        )

    def west(a):
        n = a.shape[0]
        g = ghost[n]
        minus = pltpu.roll(a, 1, 0)
        return jnp.concatenate(
            [minus[:, :cols], jnp.where(g, pltpu.roll(a[:, cols:], n - 1, 0), minus[:, cols:])], axis=1
        )

    def north(a):
        g = ghost[a.shape[0]]
        plus = pltpu.roll(a, cols + LANES - 1, 1)
        minus = pltpu.roll(a[:, cols - LANES :], 1, 1)[:, LANES:]
        return jnp.concatenate([plus[:, :cols], jnp.where(g, minus, plus[:, cols:])], axis=1)

    def south(a):
        g = ghost[a.shape[0]]
        minus = pltpu.roll(a, 1, 1)
        plus = pltpu.roll(a[:, cols:], LANES - 1, 1)
        return jnp.concatenate([minus[:, :cols], jnp.where(g, plus, minus[:, cols:])], axis=1)

    return east, west, north, south


def main_kernel(
    place, fields, thick, vu, vv, east_in, west_in, north_in, south_in,
    out_eta, out_bu, out_bv, out_h, out_u, out_v, wide, deep,
):
    layers, rows, cols = thick.shape
    tall = rows + 2 * HALO
    short = rows + EDGE
    top = place[2] == 1
    bottom = place[3] == 1
    lanes = {n: lax.broadcasted_iota(jnp.int32, (n, LANES), 1) for n in (tall, short)}
    ghost = {n: jnp.logical_and(top, lanes[n] < LANES // 2) for n in (tall, short)}
    east, west, north, south = make_neighbours(ghost, cols)

    pack_n = north_in[0:tall, :]
    pack_s = jnp.where(bottom, 0.0, south_in[0:tall, :])
    for f in range(FIELDS):
        fill_fields(wide, f, fields, east_in, west_in, rows)
        up = pltpu.roll(pack_n, (-f * SLOT) % LANES, 1)
        down = pltpu.roll(pack_s, (LANES - SLOT - f * SLOT) % LANES, 1)
        edge = jnp.where(lanes[tall] >= LANES - SLOT, down, 0.0)
        wide[f, :, cols:] = jnp.where(lanes[tall] < SLOT, up, edge)
    deep_n = north_in[tall : tall + short, :]
    deep_s = jnp.where(bottom, 0.0, south_in[tall : tall + short, :])
    for k in range(layers):
        fill_layers(deep, k, layers, thick, vu, vv, east_in, west_in, rows)
    for k in range(3 * layers):
        up = pltpu.roll(deep_n, (-2 * k) % LANES, 1)
        down = pltpu.roll(deep_s, (LANES - 2 - 2 * k) % LANES, 1)
        edge = jnp.where(lanes[short] >= LANES - 2, down, 0.0)
        deep[k, :, cols:] = jnp.where(lanes[short] < 2, up, edge)

    near = lax.broadcasted_iota(jnp.int32, (EDGE, cols + LANES), 0) < EDGE // 2

    def shorten(a):
        return jnp.concatenate([a[:rows], jnp.where(near, a[rows : rows + EDGE], a[tall - EDGE :])], axis=0)

    total = wide[3]
    wave = (WAVE_LIMIT / layers) * total
    total_short = shorten(total)
    depth_u = (total_short + east(total_short)) * 0.5
    depth_v = (total_short + north(total_short)) * 0.5
    depth_u = 1.0 / jnp.where(depth_u > 0.0, depth_u, 1.0)
    depth_v = 1.0 / jnp.where(depth_v > 0.0, depth_v, 1.0)
    mask_u = wide[4]
    mask_v = wide[5]
    short_mask_u = shorten(mask_u)
    short_mask_v = shorten(mask_v)
    stress_x = wide[6]
    stress_y = wide[7]
    eta = wide[0]
    bu = wide[1]
    bv = wide[2]
    for step in range(STEPS):
        sum_u = jnp.zeros_like(bu)
        sum_v = jnp.zeros_like(bv)
        for _ in range(NSUB):
            eta = eta - (bu - west(bu) + bv - south(bv))
            bu = mask_u * (bu - wave * (east(eta) - eta) + stress_x)
            bv = mask_v * (bv - wave * (north(eta) - eta) + stress_y)
            sum_u = sum_u + bu
            sum_v = sum_v + bv
        mean_u = shorten(sum_u) * (1.0 / NSUB)
        mean_v = shorten(sum_v) * (1.0 / NSUB)
        last = step == STEPS - 1

        def first_pass(k, carry):
            press_u, press_v, total_u, total_v = carry
            h = deep[k]
            u = deep[layers + k]
            v = deep[2 * layers + k]
            east_h = east(h)
            north_h = north(h)
            thick_u = (h + east_h) * 0.5
            thick_v = (h + north_h) * 0.5
            press_u = press_u + (east_h - h)
            press_v = press_v + (north_h - h)
            trial_u = u - PRESS_COEF * press_u
            trial_v = v - PRESS_COEF * press_v
            flux_u = u * thick_u
            flux_v = v * thick_v
            new = h - FLUX_STEP * (flux_u - west(flux_u) + flux_v - south(flux_v))
            if last:
                out_h[k] = new[:rows, :cols]
            else:
                deep[k] = new
            deep[layers + k] = trial_u
            deep[2 * layers + k] = trial_v
            return press_u, press_v, total_u + thick_u * trial_u, total_v + thick_v * trial_v

        zero = jnp.zeros((short, cols + LANES), jnp.float32)
        _, _, total_u, total_v = lax.fori_loop(0, layers, first_pass, (zero, zero, zero, zero))
        fix_u = (mean_u - total_u) * depth_u
        fix_v = (mean_v - total_v) * depth_v

        def second_pass(k, carry):
            new_u = short_mask_u * (deep[layers + k] + fix_u)
            new_v = short_mask_v * (deep[2 * layers + k] + fix_v)
            if last:
                out_u[k] = new_u[:rows, :cols]
                out_v[k] = new_v[:rows, :cols]
            else:
                deep[layers + k] = new_u
                deep[2 * layers + k] = new_v
            return carry

        lax.fori_loop(0, layers, second_pass, 0)
    out_eta[...] = eta[:rows, :cols]
    out_bu[...] = bu[:rows, :cols]
    out_bv[...] = bv[:rows, :cols]


def body(
    height,
    transport_u,
    transport_v,
    thickness,
    velocity_u,
    velocity_v,
    sea_faces,
    wind_seeds,
    wind_scale,
    wind_base,
):
    layers, rows, cols = thickness.shape
    f32 = jnp.float32
    zonal = lax.axis_size("zonal")
    merid = lax.axis_size("merid")
    z = lax.axis_index("zonal")
    m = lax.axis_index("merid")
    tall = rows + 2 * HALO
    short = rows + EDGE
    place = jnp.stack([z, m, (m == merid - 1).astype(jnp.int32), (m == 0).astype(jnp.int32)]).astype(jnp.int32)

    fields, to_west, to_east = pl.pallas_call(
        lambda *refs: prepare_kernel(rows * zonal, cols * merid, *refs),
        out_shape=(
            jax.ShapeDtypeStruct((FIELDS, rows, cols), f32),
            jax.ShapeDtypeStruct((east_rows(layers), cols), f32),
            jax.ShapeDtypeStruct((west_rows(layers), cols), f32),
        ),
        in_specs=[SMEM, SMEM, SMEM] + [VMEM] * 8,
        out_specs=(VMEM, VMEM, VMEM),
        name="prepare",
    )(place, wind_seeds, wind_scale, height, transport_u, transport_v, thickness, velocity_u, velocity_v, sea_faces, wind_base)

    up = [(i, (i + 1) % zonal) for i in range(zonal)]
    down = [(j, i) for i, j in up]
    east = lax.ppermute(to_west, "zonal", down)
    west = lax.ppermute(to_east, "zonal", up)

    tile_last = cols // LANES - 1
    edge_inputs = (fields, thickness, velocity_u, velocity_v, east, west)

    def edge_specs(tile):
        return [
            pl.BlockSpec(a.shape[:-1] + (LANES,), lambda i, n=a.ndim: (0,) * (n - 1) + (tile,)) for a in edge_inputs
        ]

    pack_shape = jax.ShapeDtypeStruct((tall + short, LANES), f32)
    low, high, fold = pl.pallas_call(
        pack_kernel,
        grid=(1,),
        out_shape=(pack_shape, pack_shape, pack_shape),
        in_specs=[SMEM] + edge_specs(0) + edge_specs(tile_last),
        out_specs=(pl.BlockSpec((tall + short, LANES), lambda i: (0, 0)),) * 3,
        scratch_shapes=[
            pltpu.VMEM((FIELDS, tall, LANES), f32),
            pltpu.VMEM((3 * layers, short, LANES), f32),
        ],
        name="pack",
    )(place, *edge_inputs, *edge_inputs)

    mirror = [(i * merid + merid - 1, (zonal - 1 - i) * merid + merid - 1) for i in range(zonal)]
    folded = lax.ppermute(fold, ("zonal", "merid"), mirror)
    if merid == 2:
        swapped = lax.ppermute(jnp.where(m == 0, high, low), "merid", [(0, 1), (1, 0)])
        from_north = swapped
        from_south = swapped
    else:
        from_north = lax.ppermute(low, "merid", [(i + 1, i) for i in range(merid - 1)])
        from_south = lax.ppermute(high, "merid", [(i, i + 1) for i in range(merid - 1)])
    from_north = jnp.where(m == merid - 1, folded, from_north)

    flat = jax.ShapeDtypeStruct((rows, cols), f32)
    full = jax.ShapeDtypeStruct((layers, rows, cols), f32)
    return pl.pallas_call(
        main_kernel,
        out_shape=(flat, flat, flat, full, full, full),
        in_specs=[SMEM] + [VMEM] * 8,
        out_specs=(VMEM,) * 6,
        scratch_shapes=[
            pltpu.VMEM((FIELDS, tall, cols + LANES), f32),
            pltpu.VMEM((3 * layers, short, cols + LANES), f32),
        ],
        name="advance",
    )(place, fields, thickness, velocity_u, velocity_v, east, west, from_north, from_south)


def solution(mesh):
    placed = (
        P(("members", "zonal"), "merid"),
        P(("members", "zonal"), "merid"),
        P(("members", "zonal"), "merid"),
        P(None, ("members", "zonal"), "merid"),
        P(None, ("members", "zonal"), "merid"),
        P(None, ("members", "zonal"), "merid"),
        P(None, "zonal", "merid"),
        P("members", None),
        P("members"),
        P(None, "zonal", "merid"),
    )
    return jax.shard_map(
        body,
        mesh=mesh,
        in_specs=placed,
        out_specs=(
            P(("members", "zonal"), "merid"),
            P(("members", "zonal"), "merid"),
            P(("members", "zonal"), "merid"),
            P(None, ("members", "zonal"), "merid"),
            P(None, ("members", "zonal"), "merid"),
            P(None, ("members", "zonal"), "merid"),
        ),
        check_vma=False,
    )
```

```python
import math

import jax
import jax.numpy as jnp
from jax import lax
from jax.experimental import pallas as pl
from jax.experimental.pallas import tpu as pltpu
from jax.sharding import PartitionSpec as P


NSUB = 6
STEPS = 2
WAVE_LIMIT = 0.225
STRESS_SCALE = 0.1
FLUX_STEP = 0.05
PRESS_COEF = 0.05

FIELDS = 8
HALO = NSUB * STEPS
SLOT = 16
LANES = 128
EDGE = 8

VMEM = pl.BlockSpec(memory_space=pltpu.VMEM)
SMEM = pl.BlockSpec(memory_space=pltpu.SMEM)


def whole_mod(product, total):
    rest = product - jnp.floor(product * (1.0 / total)) * total
    rest = jnp.where(rest < 0.0, rest + total, rest)
    return jnp.where(rest >= total, rest - total, rest)


def prepare_kernel(
    total_x, total_y, seeds, scale, eta, bu, bv, thick, vu, vv, faces, base,
    fields, to_west, to_east, packs, strips_west, strips_east,
):
    layers, rows, cols = thick.shape
    modes = scale.shape[0]
    f32 = jnp.float32

    lane = lax.broadcasted_iota(jnp.int32, (rows, LANES), 1)
    sub = lax.broadcasted_iota(jnp.int32, (8, cols), 0)
    wave_x = jnp.zeros((rows, LANES), f32)
    wave_y = jnp.zeros((8, cols), f32)
    for m in range(modes):
        wave_x = jnp.where(lane == m, seeds[0, m].astype(f32), wave_x)
        wave_y = jnp.where(sub == m, seeds[1, m].astype(f32), wave_y)
    col = (lax.broadcasted_iota(jnp.int32, (rows, LANES), 0) + lax.axis_index("zonal") * rows).astype(f32)
    row = (lax.broadcasted_iota(jnp.int32, (8, cols), 1) + lax.axis_index("merid") * cols).astype(f32)
    angle_x = whole_mod(wave_x * col, total_x) * (2.0 * math.pi / total_x)
    angle_y = whole_mod(wave_y * row, total_y) * (2.0 * math.pi / total_y)
    cos_x, sin_x = jnp.cos(angle_x), jnp.sin(angle_x)
    cos_y, sin_y = jnp.cos(angle_y), jnp.sin(angle_y)
    sum_cos = base[0]
    sum_sin = base[1]
    for m in range(modes):
        amp = scale[m]
        ca = cos_x[:, m : m + 1] * amp
        sa = sin_x[:, m : m + 1] * amp
        cb = cos_y[m : m + 1, :]
        sb = sin_y[m : m + 1, :]
        sum_cos = sum_cos + (ca * cb - sa * sb)
        sum_sin = sum_sin + (sa * cb + ca * sb)
    fields[0] = eta[...]
    fields[1] = bu[...]
    fields[2] = bv[...]
    total = thick[0]
    for k in range(1, layers):
        total = total + thick[k]
    fields[3] = total
    fields[4] = faces[0].astype(f32)
    fields[5] = faces[1].astype(f32)
    fields[6] = STRESS_SCALE * sum_cos
    fields[7] = STRESS_SCALE * sum_sin
    for f in range(FIELDS):
        value = fields[f]
        to_west[f * HALO : (f + 1) * HALO, :] = value[:HALO]
        to_east[f * HALO : (f + 1) * HALO, :] = value[rows - HALO :]
    for side, low in enumerate((True, False)):
        tile = slice(0, LANES) if low else slice(cols - LANES, cols)
        acc = jnp.zeros((rows, LANES), f32)
        for f in range(FIELDS):
            moved = pltpu.roll(fields[f, :, tile], (f * SLOT + (0 if low else SLOT)) % LANES, 1)
            acc = jnp.where(lane // SLOT == f, moved, acc)
        deep = jnp.zeros((rows, LANES), f32)
        for s, own in enumerate((thick, vu, vv)):
            for k in range(layers):
                at = 2 * (s * layers + k)
                moved = pltpu.roll(own[k, :, tile], (at + (0 if low else 2)) % LANES, 1)
                deep = jnp.where(lane // 2 == s * layers + k, moved, deep)
        packs[2 * side] = acc
        packs[2 * side + 1] = deep
    for side in range(2):
        acc = packs[2 * side]
        strips_west[side * HALO : (side + 1) * HALO, :] = acc[:HALO]
        strips_east[side * HALO : (side + 1) * HALO, :] = acc[rows - HALO :]
        deep = packs[2 * side + 1]
        strips_west[2 * HALO + side : 2 * HALO + side + 1, :] = deep[:1]
        strips_east[2 * HALO + side : 2 * HALO + side + 1, :] = deep[rows - 1 :]
    used = 2 * HALO + 2
    strips_west[used:, :] = jnp.zeros((strips_west.shape[0] - used, LANES), f32)
    strips_east[used:, :] = jnp.zeros((strips_east.shape[0] - used, LANES), f32)


def edges_kernel(thick, vu, vv, after, to_west, to_east):
    layers, rows, _ = thick.shape
    n = layers
    for k in range(layers):
        to_west[k : k + 1, :] = thick[k, 0:1, :]
        to_west[n + k : n + k + 1, :] = vu[k, 0:1, :] * ((thick[k, 0:1, :] + thick[k, 1:2, :]) * 0.5)
        to_west[2 * n + k : 2 * n + k + 1, :] = vv[k, 0:1, :]
        near = thick[k, rows - 2 : rows - 1, :]
        last = thick[k, rows - 1 : rows, :]
        to_east[k : k + 1, :] = last
        to_east[n + k : n + k + 1, :] = vu[k, rows - 2 : rows - 1, :] * ((near + last) * 0.5)
        to_east[2 * n + k : 2 * n + k + 1, :] = vu[k, rows - 1 : rows, :]
        to_east[3 * n + k : 3 * n + k + 1, :] = vv[k, rows - 1 : rows, :]


def fill_fields(target, f, fields, east, west, rows):
    cols = fields.shape[-1]
    target[f, 0:rows, 0:cols] = fields[f]
    target[f, rows : rows + HALO, 0:cols] = east[f * HALO : (f + 1) * HALO, :]
    target[f, rows + HALO : rows + 2 * HALO, 0:cols] = west[f * HALO : (f + 1) * HALO, :]


def fill_layers(target, k, layers, thick, vu, vv, east, west, rows):
    cols = thick.shape[-1]
    n = layers
    e, w = rows, rows + EDGE
    zero = jnp.zeros((EDGE, cols), jnp.float32)
    for s, own in enumerate((thick, vu, vv)):
        target[s * n + k, 0:rows, 0:cols] = own[k]
        target[s * n + k, rows : rows + EDGE, 0:cols] = zero
    target[k, e : e + 1, 0:cols] = east[k : k + 1, :]
    target[k, w - 1 : w, 0:cols] = west[k : k + 1, :]
    target[n + k, e : e + 1, 0:cols] = east[n + k : n + k + 1, :]
    target[n + k, w - 2 : w - 1, 0:cols] = west[n + k : n + k + 1, :]
    target[n + k, w - 1 : w, 0:cols] = west[2 * n + k : 2 * n + k + 1, :]
    target[2 * n + k, e : e + 1, 0:cols] = east[2 * n + k : 2 * n + k + 1, :]
    target[2 * n + k, w - 1 : w, 0:cols] = west[3 * n + k : 3 * n + k + 1, :]


def flipped(pack, rows, group):
    size = pack.shape[0]
    q = lax.broadcasted_iota(jnp.int32, (size, size), 0)
    p = lax.broadcasted_iota(jnp.int32, (size, size), 1)
    source = rows - 1 - q
    source = jnp.where(source < 0, source + size, source)
    flip_rows = (p == source).astype(jnp.float32)
    a = lax.broadcasted_iota(jnp.int32, (LANES, LANES), 0)
    b = lax.broadcasted_iota(jnp.int32, (LANES, LANES), 1)
    inner = jnp.bitwise_and(b, group - 1)
    flip_lanes = (a == b - inner + (group - 1 - inner)).astype(jnp.float32)
    half = jnp.dot(flip_rows, pack, precision=lax.Precision.HIGHEST, preferred_element_type=jnp.float32)
    return jnp.dot(half, flip_lanes, precision=lax.Precision.HIGHEST, preferred_element_type=jnp.float32)


def pack_kernel(merid, packs, east, west, swap, high, fold):
    rows = packs.shape[1]
    tall = rows + 2 * HALO
    short = rows + EDGE
    at_bottom = lax.axis_index("merid") == 0
    both = []
    for side in range(2):
        acc = jnp.concatenate(
            [packs[2 * side], east[side * HALO : (side + 1) * HALO, :], west[side * HALO : (side + 1) * HALO, :]], axis=0
        )
        high[tall : tall + rows, :] = packs[2 * side + 1]
        high[tall + rows :, :] = jnp.zeros((EDGE, LANES), jnp.float32)
        row = 2 * HALO + side
        high[tall + rows : tall + rows + 1, :] = east[row : row + 1, :]
        high[tall + short - 1 : tall + short, :] = west[row : row + 1, :]
        both.append((acc, high[tall : tall + short, :]))
    (low_f, low_l), (high_f, high_l) = both
    high[0:tall, :] = high_f
    if merid == 2:
        low_f = jnp.where(at_bottom, high_f, low_f)
        low_l = jnp.where(at_bottom, high_l, low_l)
    swap[0:tall, :] = low_f
    swap[tall : tall + short, :] = low_l
    fold[0:tall, :] = flipped(high_f, rows, SLOT)
    fold[tall : tall + short, :] = flipped(high_l, rows, 2)


def make_neighbours(ghost, cols):
    def east(a):
        n = a.shape[0]
        g = ghost[n]
        plus = pltpu.roll(a, n - 1, 0)
        return jnp.concatenate(
            [plus[:, :cols], jnp.where(g, pltpu.roll(a[:, cols:], 1, 0), plus[:, cols:])], axis=1
        )

    def west(a):
        n = a.shape[0]
        g = ghost[n]
        minus = pltpu.roll(a, 1, 0)
        return jnp.concatenate(
            [minus[:, :cols], jnp.where(g, pltpu.roll(a[:, cols:], n - 1, 0), minus[:, cols:])], axis=1
        )

    def north(a):
        g = ghost[a.shape[0]]
        plus = pltpu.roll(a, cols + LANES - 1, 1)
        minus = pltpu.roll(a[:, cols - LANES :], 1, 1)[:, LANES:]
        return jnp.concatenate([plus[:, :cols], jnp.where(g, minus, plus[:, cols:])], axis=1)

    def south(a):
        g = ghost[a.shape[0]]
        minus = pltpu.roll(a, 1, 1)
        plus = pltpu.roll(a[:, cols:], LANES - 1, 1)
        return jnp.concatenate([minus[:, :cols], jnp.where(g, plus, minus[:, cols:])], axis=1)

    return east, west, north, south


def setting(merid, sizes, cols):
    m = lax.axis_index("merid")
    top = m == merid - 1
    lanes = {n: lax.broadcasted_iota(jnp.int32, (n, LANES), 1) for n in sizes}
    ghost = {n: jnp.logical_and(top, lanes[n] < LANES // 2) for n in sizes}
    return m == 0, top, lanes, make_neighbours(ghost, cols)


def wide_kernel(
    merid, layers, fields, east_in, west_in, north_in, south_in, fold_in, out_eta, out_bu, out_bv, shared, wide,
):
    _, rows, cols = fields.shape
    tall = rows + 2 * HALO
    short = rows + EDGE
    bottom, top, lanes, (east, west, north, south) = setting(merid, (tall, short), cols)

    pack_n = jnp.where(top, fold_in[0:tall, :], north_in[0:tall, :])
    pack_s = jnp.where(bottom, 0.0, south_in[0:tall, :])
    for f in range(FIELDS):
        fill_fields(wide, f, fields, east_in, west_in, rows)
        up = pltpu.roll(pack_n, (-f * SLOT) % LANES, 1)
        down = pltpu.roll(pack_s, (LANES - SLOT - f * SLOT) % LANES, 1)
        edge = jnp.where(lanes[tall] >= LANES - SLOT, down, 0.0)
        wide[f, :, cols:] = jnp.where(lanes[tall] < SLOT, up, edge)

    near = lax.broadcasted_iota(jnp.int32, (EDGE, cols + LANES), 0) < EDGE // 2

    def shorten(a):
        return jnp.concatenate([a[:rows], jnp.where(near, a[rows : rows + EDGE], a[tall - EDGE :])], axis=0)

    total = wide[3]
    total_short = shorten(total)
    depth_u = (total_short + east(total_short)) * 0.5
    depth_v = (total_short + north(total_short)) * 0.5
    shared[0] = 1.0 / jnp.where(depth_u > 0.0, depth_u, 1.0)
    shared[1] = 1.0 / jnp.where(depth_v > 0.0, depth_v, 1.0)
    shared[2] = shorten(wide[4])
    shared[3] = shorten(wide[5])
    wide[3] = (WAVE_LIMIT / layers) * total
    eta = wide[0]
    bu = wide[1]
    bv = wide[2]
    for step in range(STEPS):
        sum_u = jnp.zeros_like(bu)
        sum_v = jnp.zeros_like(bv)
        for _ in range(NSUB):
            eta = eta - (bu - west(bu) + bv - south(bv))
            bu = wide[4] * (bu - wide[3] * (east(eta) - eta) + wide[6])
            bv = wide[5] * (bv - wide[3] * (north(eta) - eta) + wide[7])
            sum_u = sum_u + bu
            sum_v = sum_v + bv
        shared[4 + 2 * step] = shorten(sum_u) * (1.0 / NSUB)
        shared[5 + 2 * step] = shorten(sum_v) * (1.0 / NSUB)
    out_eta[...] = eta[:rows, :cols]
    out_bu[...] = bu[:rows, :cols]
    out_bv[...] = bv[:rows, :cols]


def layers_kernel(
    merid, thick, vu, vv, east_in, west_in, north_in, south_in, fold_in, shared, out_h, out_u, out_v, deep,
):
    layers, rows, cols = thick.shape
    tall = rows + 2 * HALO
    short = rows + EDGE
    bottom, top, lanes, (east, west, north, south) = setting(merid, (short,), cols)
    deep_n = jnp.where(top, fold_in[tall : tall + short, :], north_in[tall : tall + short, :])
    deep_s = jnp.where(bottom, 0.0, south_in[tall : tall + short, :])
    for k in range(layers):
        fill_layers(deep, k, layers, thick, vu, vv, east_in, west_in, rows)
    for k in range(3 * layers):
        up = pltpu.roll(deep_n, (-2 * k) % LANES, 1)
        down = pltpu.roll(deep_s, (LANES - 2 - 2 * k) % LANES, 1)
        edge = jnp.where(lanes[short] >= LANES - 2, down, 0.0)
        deep[k, :, cols:] = jnp.where(lanes[short] < 2, up, edge)
    spot = lax.broadcasted_iota(jnp.int32, (short, cols), 0)
    given = jnp.logical_or(spot == rows, spot == short - 2)

    for step in range(STEPS):
        last = step == STEPS - 1

        def first_pass(k, carry):
            press_u, press_v, total_u, total_v = carry
            h = deep[k]
            u = deep[layers + k]
            v = deep[2 * layers + k]
            east_h = east(h)
            north_h = north(h)
            thick_u = (h + east_h) * 0.5
            thick_v = (h + north_h) * 0.5
            press_u = press_u + (east_h - h)
            press_v = press_v + (north_h - h)
            trial_u = u - PRESS_COEF * press_u
            trial_v = v - PRESS_COEF * press_v
            flux_u = u * thick_u
            if not last:
                flux_u = jnp.concatenate([jnp.where(given, u[:, :cols], flux_u[:, :cols]), flux_u[:, cols:]], axis=1)
            flux_v = v * thick_v
            new = h - FLUX_STEP * (flux_u - west(flux_u) + flux_v - south(flux_v))
            if last:
                out_h[k] = new[:rows, :cols]
            else:
                deep[k] = new
            deep[layers + k] = trial_u
            deep[2 * layers + k] = trial_v
            return press_u, press_v, total_u + thick_u * trial_u, total_v + thick_v * trial_v

        zero = jnp.zeros((short, cols + LANES), jnp.float32)
        _, _, total_u, total_v = lax.fori_loop(0, layers, first_pass, (zero, zero, zero, zero))
        fix_u = (shared[4 + 2 * step] - total_u) * shared[0]
        fix_v = (shared[5 + 2 * step] - total_v) * shared[1]

        def second_pass(k, carry):
            new_u = shared[2] * (deep[layers + k] + fix_u)
            new_v = shared[3] * (deep[2 * layers + k] + fix_v)
            if last:
                out_u[k] = new_u[:rows, :cols]
                out_v[k] = new_v[:rows, :cols]
            else:
                deep[layers + k] = new_u
                deep[2 * layers + k] = new_v
            return carry

        lax.fori_loop(0, layers, second_pass, 0)


def body(
    height,
    transport_u,
    transport_v,
    thickness,
    velocity_u,
    velocity_v,
    sea_faces,
    wind_seeds,
    wind_scale,
    wind_base,
):
    layers, rows, cols = thickness.shape
    f32 = jnp.float32
    zonal = lax.axis_size("zonal")
    merid = lax.axis_size("merid")
    tall = rows + 2 * HALO
    short = rows + EDGE

    def shape(*dims):
        return jax.ShapeDtypeStruct(dims, f32)

    fields, wide_west, wide_east, packs, strips_west, strips_east = pl.pallas_call(
        lambda *refs: prepare_kernel(rows * zonal, cols * merid, *refs),
        out_shape=(
            shape(FIELDS, rows, cols),
            shape(FIELDS * HALO, cols),
            shape(FIELDS * HALO, cols),
            shape(4, rows, LANES),
            shape(2 * HALO + EDGE, LANES),
            shape(2 * HALO + EDGE, LANES),
        ),
        in_specs=[SMEM, SMEM] + [VMEM] * 8,
        out_specs=(VMEM,) * 6,
        name="prepare",
    )(wind_seeds.T, wind_scale, height, transport_u, transport_v, thickness, velocity_u, velocity_v, sea_faces, wind_base)

    up = [(i, (i + 1) % zonal) for i in range(zonal)]
    down = [(j, i) for i, j in up]
    strips_from_east = lax.ppermute(strips_west, "zonal", down)
    strips_from_west = lax.ppermute(strips_east, "zonal", up)
    wide_from_east = lax.ppermute(wide_west, "zonal", down)
    wide_from_west = lax.ppermute(wide_east, "zonal", up)

    deep_west, deep_east = pl.pallas_call(
        edges_kernel,
        out_shape=(shape(3 * layers, cols), shape(4 * layers, cols)),
        in_specs=[VMEM] * 3 + [pl.BlockSpec(memory_space=pl.ANY)],
        out_specs=(VMEM, VMEM),
        name="edges",
    )(thickness, velocity_u, velocity_v, strips_west)
    deep_from_east = lax.ppermute(deep_west, "zonal", down)
    deep_from_west = lax.ppermute(deep_east, "zonal", up)

    swap, high, fold = pl.pallas_call(
        lambda *refs: pack_kernel(merid, *refs),
        out_shape=(shape(tall + short, LANES),) * 3,
        in_specs=[VMEM] * 3,
        out_specs=(VMEM,) * 3,
        name="pack",
    )(packs, strips_from_east, strips_from_west)

    mirror = [(i * merid + merid - 1, (zonal - 1 - i) * merid + merid - 1) for i in range(zonal)]
    folded = lax.ppermute(fold, ("zonal", "merid"), mirror)
    if merid == 2:
        from_north = lax.ppermute(swap, "merid", [(0, 1), (1, 0)])
        from_south = from_north
    else:
        from_north = lax.ppermute(swap, "merid", [(i + 1, i) for i in range(merid - 1)])
        from_south = lax.ppermute(high, "merid", [(i, i + 1) for i in range(merid - 1)])

    flat = shape(rows, cols)
    full = shape(layers, rows, cols)
    eta, bu, bv, shared = pl.pallas_call(
        lambda *refs: wide_kernel(merid, layers, *refs),
        out_shape=(flat, flat, flat, shape(4 + 2 * STEPS, short, cols + LANES)),
        in_specs=[VMEM] * 6,
        out_specs=(VMEM,) * 4,
        scratch_shapes=[pltpu.VMEM((FIELDS, tall, cols + LANES), f32)],
        name="barotropic",
    )(fields, wide_from_east, wide_from_west, from_north, from_south, folded)
    h, u, v = pl.pallas_call(
        lambda *refs: layers_kernel(merid, *refs),
        out_shape=(full, full, full),
        in_specs=[VMEM] * 9,
        out_specs=(VMEM,) * 3,
        scratch_shapes=[pltpu.VMEM((3 * layers, short, cols + LANES), f32)],
        name="layers",
    )(thickness, velocity_u, velocity_v, deep_from_east, deep_from_west, from_north, from_south, folded, shared)
    return eta, bu, bv, h, u, v


def solution(mesh):
    placed = (
        P(("members", "zonal"), "merid"),
        P(("members", "zonal"), "merid"),
        P(("members", "zonal"), "merid"),
        P(None, ("members", "zonal"), "merid"),
        P(None, ("members", "zonal"), "merid"),
        P(None, ("members", "zonal"), "merid"),
        P(None, "zonal", "merid"),
        P("members", None),
        P("members"),
        P(None, "zonal", "merid"),
    )

    return jax.shard_map(
        body,
        mesh=mesh,
        in_specs=placed,
        out_specs=(
            P(("members", "zonal"), "merid"),
            P(("members", "zonal"), "merid"),
            P(("members", "zonal"), "merid"),
            P(None, ("members", "zonal"), "merid"),
            P(None, ("members", "zonal"), "merid"),
            P(None, ("members", "zonal"), "merid"),
        ),
        check_vma=False,
    )
```

```python
import math

import jax
import jax.numpy as jnp
from jax import lax
from jax.experimental import pallas as pl
from jax.experimental.pallas import tpu as pltpu
from jax.sharding import PartitionSpec as P


NSUB = 6
STEPS = 2
WAVE_LIMIT = 0.225
STRESS_SCALE = 0.1
FLUX_STEP = 0.05
PRESS_COEF = 0.05

FIELDS = 8
HALO = NSUB * STEPS
SLOT = 16
LANES = 128
EDGE = 8

VMEM = pl.BlockSpec(memory_space=pltpu.VMEM)
SMEM = pl.BlockSpec(memory_space=pltpu.SMEM)


def whole_mod(product, total):
    rest = product - jnp.floor(product * (1.0 / total)) * total
    rest = jnp.where(rest < 0.0, rest + total, rest)
    return jnp.where(rest >= total, rest - total, rest)


def prepare_kernel(
    total_x, total_y, seeds, scale, eta, bu, bv, thick, vu, vv, faces, base,
    fields, to_west, to_east, packs, strips_west, strips_east,
):
    layers, rows, cols = thick.shape
    modes = scale.shape[0]
    f32 = jnp.float32

    lane = lax.broadcasted_iota(jnp.int32, (rows, LANES), 1)
    sub = lax.broadcasted_iota(jnp.int32, (8, cols), 0)
    wave_x = jnp.zeros((rows, LANES), f32)
    wave_y = jnp.zeros((8, cols), f32)
    for m in range(modes):
        wave_x = jnp.where(lane == m, seeds[0, m].astype(f32), wave_x)
        wave_y = jnp.where(sub == m, seeds[1, m].astype(f32), wave_y)
    col = (lax.broadcasted_iota(jnp.int32, (rows, LANES), 0) + lax.axis_index("zonal") * rows).astype(f32)
    row = (lax.broadcasted_iota(jnp.int32, (8, cols), 1) + lax.axis_index("merid") * cols).astype(f32)
    angle_x = whole_mod(wave_x * col, total_x) * (2.0 * math.pi / total_x)
    angle_y = whole_mod(wave_y * row, total_y) * (2.0 * math.pi / total_y)
    cos_x, sin_x = jnp.cos(angle_x), jnp.sin(angle_x)
    cos_y, sin_y = jnp.cos(angle_y), jnp.sin(angle_y)
    sum_cos = base[0]
    sum_sin = base[1]
    for m in range(modes):
        amp = scale[m]
        ca = cos_x[:, m : m + 1] * amp
        sa = sin_x[:, m : m + 1] * amp
        cb = cos_y[m : m + 1, :]
        sb = sin_y[m : m + 1, :]
        sum_cos = sum_cos + (ca * cb - sa * sb)
        sum_sin = sum_sin + (sa * cb + ca * sb)
    fields[0] = eta[...]
    fields[1] = bu[...]
    fields[2] = bv[...]
    total = thick[0]
    for k in range(1, layers):
        total = total + thick[k]
    fields[3] = total
    fields[4] = faces[0].astype(f32)
    fields[5] = faces[1].astype(f32)
    fields[6] = STRESS_SCALE * sum_cos
    fields[7] = STRESS_SCALE * sum_sin
    for f in range(FIELDS):
        value = fields[f]
        to_west[f * HALO : (f + 1) * HALO, :] = value[:HALO]
        to_east[f * HALO : (f + 1) * HALO, :] = value[rows - HALO :]
    start = FIELDS * HALO
    edge_rows(thick, vu, vv, to_west.at[pl.ds(start, 3 * layers)], to_east.at[pl.ds(start, 4 * layers)])
    for side, low in enumerate((True, False)):
        tile = slice(0, LANES) if low else slice(cols - LANES, cols)
        acc = jnp.zeros((rows, LANES), f32)
        for f in range(FIELDS):
            moved = pltpu.roll(fields[f, :, tile], (f * SLOT + (0 if low else SLOT)) % LANES, 1)
            acc = jnp.where(lane // SLOT == f, moved, acc)
        deep = jnp.zeros((rows, LANES), f32)
        for s, own in enumerate((thick, vu, vv)):
            for k in range(layers):
                at = 2 * (s * layers + k)
                moved = pltpu.roll(own[k, :, tile], (at + (0 if low else 2)) % LANES, 1)
                deep = jnp.where(lane // 2 == s * layers + k, moved, deep)
        packs[2 * side] = acc
        packs[2 * side + 1] = deep
    for side in range(2):
        acc = packs[2 * side]
        strips_west[side * HALO : (side + 1) * HALO, :] = acc[:HALO]
        strips_east[side * HALO : (side + 1) * HALO, :] = acc[rows - HALO :]
        deep = packs[2 * side + 1]
        strips_west[2 * HALO + side : 2 * HALO + side + 1, :] = deep[:1]
        strips_east[2 * HALO + side : 2 * HALO + side + 1, :] = deep[rows - 1 :]
    used = 2 * HALO + 2
    strips_west[used:, :] = jnp.zeros((strips_west.shape[0] - used, LANES), f32)
    strips_east[used:, :] = jnp.zeros((strips_east.shape[0] - used, LANES), f32)


def edge_rows(thick, vu, vv, to_west, to_east):
    layers, rows, _ = thick.shape
    n = layers
    for k in range(layers):
        to_west[k : k + 1, :] = thick[k, 0:1, :]
        to_west[n + k : n + k + 1, :] = vu[k, 0:1, :] * ((thick[k, 0:1, :] + thick[k, 1:2, :]) * 0.5)
        to_west[2 * n + k : 2 * n + k + 1, :] = vv[k, 0:1, :]
        near = thick[k, rows - 2 : rows - 1, :]
        last = thick[k, rows - 1 : rows, :]
        to_east[k : k + 1, :] = last
        to_east[n + k : n + k + 1, :] = vu[k, rows - 2 : rows - 1, :] * ((near + last) * 0.5)
        to_east[2 * n + k : 2 * n + k + 1, :] = vu[k, rows - 1 : rows, :]
        to_east[3 * n + k : 3 * n + k + 1, :] = vv[k, rows - 1 : rows, :]


def fill_fields(target, f, fields, east, west, rows):
    cols = fields.shape[-1]
    target[f, 0:rows, 0:cols] = fields[f]
    target[f, rows : rows + HALO, 0:cols] = east[f * HALO : (f + 1) * HALO, :]
    target[f, rows + HALO : rows + 2 * HALO, 0:cols] = west[f * HALO : (f + 1) * HALO, :]


def fill_layers(target, k, layers, thick, vu, vv, east, west, rows):
    cols = thick.shape[-1]
    n = layers
    e, w = rows, rows + EDGE
    zero = jnp.zeros((EDGE, cols), jnp.float32)
    for s, own in enumerate((thick, vu, vv)):
        target[s * n + k, 0:rows, 0:cols] = own[k]
        target[s * n + k, rows : rows + EDGE, 0:cols] = zero
    target[k, e : e + 1, 0:cols] = east[k : k + 1, :]
    target[k, w - 1 : w, 0:cols] = west[k : k + 1, :]
    target[n + k, e : e + 1, 0:cols] = east[n + k : n + k + 1, :]
    target[n + k, w - 2 : w - 1, 0:cols] = west[n + k : n + k + 1, :]
    target[n + k, w - 1 : w, 0:cols] = west[2 * n + k : 2 * n + k + 1, :]
    target[2 * n + k, e : e + 1, 0:cols] = east[2 * n + k : 2 * n + k + 1, :]
    target[2 * n + k, w - 1 : w, 0:cols] = west[3 * n + k : 3 * n + k + 1, :]


def flipped(pack, rows, group):
    size = pack.shape[0]
    q = lax.broadcasted_iota(jnp.int32, (size, size), 0)
    p = lax.broadcasted_iota(jnp.int32, (size, size), 1)
    source = rows - 1 - q
    source = jnp.where(source < 0, source + size, source)
    flip_rows = (p == source).astype(jnp.float32)
    a = lax.broadcasted_iota(jnp.int32, (LANES, LANES), 0)
    b = lax.broadcasted_iota(jnp.int32, (LANES, LANES), 1)
    inner = jnp.bitwise_and(b, group - 1)
    flip_lanes = (a == b - inner + (group - 1 - inner)).astype(jnp.float32)
    half = jnp.dot(flip_rows, pack, precision=lax.Precision.HIGHEST, preferred_element_type=jnp.float32)
    return jnp.dot(half, flip_lanes, precision=lax.Precision.HIGHEST, preferred_element_type=jnp.float32)


def pack_kernel(merid, packs, east, west, swap, high, fold):
    rows = packs.shape[1]
    tall = rows + 2 * HALO
    short = rows + EDGE
    at_bottom = lax.axis_index("merid") == 0
    both = []
    for side in range(2):
        acc = jnp.concatenate(
            [packs[2 * side], east[side * HALO : (side + 1) * HALO, :], west[side * HALO : (side + 1) * HALO, :]], axis=0
        )
        high[tall : tall + rows, :] = packs[2 * side + 1]
        high[tall + rows :, :] = jnp.zeros((EDGE, LANES), jnp.float32)
        row = 2 * HALO + side
        high[tall + rows : tall + rows + 1, :] = east[row : row + 1, :]
        high[tall + short - 1 : tall + short, :] = west[row : row + 1, :]
        both.append((acc, high[tall : tall + short, :]))
    (low_f, low_l), (high_f, high_l) = both
    high[0:tall, :] = high_f
    if merid == 2:
        low_f = jnp.where(at_bottom, high_f, low_f)
        low_l = jnp.where(at_bottom, high_l, low_l)
    swap[0:tall, :] = low_f
    swap[tall : tall + short, :] = low_l
    fold[0:tall, :] = flipped(high_f, rows, SLOT)
    fold[tall : tall + short, :] = flipped(high_l, rows, 2)


def make_neighbours(ghost, cols):
    def east(a):
        n = a.shape[0]
        g = ghost[n]
        plus = pltpu.roll(a, n - 1, 0)
        return jnp.concatenate(
            [plus[:, :cols], jnp.where(g, pltpu.roll(a[:, cols:], 1, 0), plus[:, cols:])], axis=1
        )

    def west(a):
        n = a.shape[0]
        g = ghost[n]
        minus = pltpu.roll(a, 1, 0)
        return jnp.concatenate(
            [minus[:, :cols], jnp.where(g, pltpu.roll(a[:, cols:], n - 1, 0), minus[:, cols:])], axis=1
        )

    def north(a):
        g = ghost[a.shape[0]]
        plus = pltpu.roll(a, cols + LANES - 1, 1)
        minus = pltpu.roll(a[:, cols - LANES :], 1, 1)[:, LANES:]
        return jnp.concatenate([plus[:, :cols], jnp.where(g, minus, plus[:, cols:])], axis=1)

    def south(a):
        g = ghost[a.shape[0]]
        minus = pltpu.roll(a, 1, 1)
        plus = pltpu.roll(a[:, cols:], LANES - 1, 1)
        return jnp.concatenate([minus[:, :cols], jnp.where(g, plus, minus[:, cols:])], axis=1)

    return east, west, north, south


def setting(merid, sizes, cols):
    m = lax.axis_index("merid")
    top = m == merid - 1
    lanes = {n: lax.broadcasted_iota(jnp.int32, (n, LANES), 1) for n in sizes}
    ghost = {n: jnp.logical_and(top, lanes[n] < LANES // 2) for n in sizes}
    return m == 0, top, lanes, make_neighbours(ghost, cols)


def wide_kernel(
    merid, layers, fields, east_in, west_in, north_in, south_in, fold_in, out_eta, out_bu, out_bv, shared, wide,
):
    _, rows, cols = fields.shape
    tall = rows + 2 * HALO
    short = rows + EDGE
    bottom, top, lanes, (east, west, north, south) = setting(merid, (tall, short), cols)

    pack_n = jnp.where(top, fold_in[0:tall, :], north_in[0:tall, :])
    pack_s = jnp.where(bottom, 0.0, south_in[0:tall, :])
    for f in range(FIELDS):
        fill_fields(wide, f, fields, east_in, west_in, rows)
        up = pltpu.roll(pack_n, (-f * SLOT) % LANES, 1)
        down = pltpu.roll(pack_s, (LANES - SLOT - f * SLOT) % LANES, 1)
        edge = jnp.where(lanes[tall] >= LANES - SLOT, down, 0.0)
        wide[f, :, cols:] = jnp.where(lanes[tall] < SLOT, up, edge)

    near = lax.broadcasted_iota(jnp.int32, (EDGE, cols + LANES), 0) < EDGE // 2

    def shorten(a):
        return jnp.concatenate([a[:rows], jnp.where(near, a[rows : rows + EDGE], a[tall - EDGE :])], axis=0)

    total = wide[3]
    total_short = shorten(total)
    depth_u = (total_short + east(total_short)) * 0.5
    depth_v = (total_short + north(total_short)) * 0.5
    shared[0] = 1.0 / jnp.where(depth_u > 0.0, depth_u, 1.0)
    shared[1] = 1.0 / jnp.where(depth_v > 0.0, depth_v, 1.0)
    shared[2] = shorten(wide[4])
    shared[3] = shorten(wide[5])
    wide[3] = (WAVE_LIMIT / layers) * total
    eta = wide[0]
    bu = wide[1]
    bv = wide[2]
    for step in range(STEPS):
        sum_u = jnp.zeros_like(bu)
        sum_v = jnp.zeros_like(bv)
        for _ in range(NSUB):
            eta = eta - (bu - west(bu) + bv - south(bv))
            bu = wide[4] * (bu - wide[3] * (east(eta) - eta) + wide[6])
            bv = wide[5] * (bv - wide[3] * (north(eta) - eta) + wide[7])
            sum_u = sum_u + bu
            sum_v = sum_v + bv
        shared[4 + 2 * step] = shorten(sum_u) * (1.0 / NSUB)
        shared[5 + 2 * step] = shorten(sum_v) * (1.0 / NSUB)
    out_eta[...] = eta[:rows, :cols]
    out_bu[...] = bu[:rows, :cols]
    out_bv[...] = bv[:rows, :cols]


def layers_kernel(
    merid, thick, vu, vv, east_in, west_in, north_in, south_in, fold_in, shared, out_h, out_u, out_v, deep,
):
    layers, rows, cols = thick.shape
    tall = rows + 2 * HALO
    short = rows + EDGE
    bottom, top, lanes, (east, west, north, south) = setting(merid, (short,), cols)
    deep_n = jnp.where(top, fold_in[tall : tall + short, :], north_in[tall : tall + short, :])
    deep_s = jnp.where(bottom, 0.0, south_in[tall : tall + short, :])
    for k in range(layers):
        fill_layers(deep, k, layers, thick, vu, vv, east_in, west_in, rows)
    for k in range(3 * layers):
        up = pltpu.roll(deep_n, (-2 * k) % LANES, 1)
        down = pltpu.roll(deep_s, (LANES - 2 - 2 * k) % LANES, 1)
        edge = jnp.where(lanes[short] >= LANES - 2, down, 0.0)
        deep[k, :, cols:] = jnp.where(lanes[short] < 2, up, edge)
    spot = lax.broadcasted_iota(jnp.int32, (short, cols), 0)
    given = jnp.logical_or(spot == rows, spot == short - 2)

    for step in range(STEPS):
        last = step == STEPS - 1

        def first_pass(k, carry):
            press_u, press_v, total_u, total_v = carry
            h = deep[k]
            u = deep[layers + k]
            v = deep[2 * layers + k]
            east_h = east(h)
            north_h = north(h)
            thick_u = (h + east_h) * 0.5
            thick_v = (h + north_h) * 0.5
            press_u = press_u + (east_h - h)
            press_v = press_v + (north_h - h)
            trial_u = u - PRESS_COEF * press_u
            trial_v = v - PRESS_COEF * press_v
            flux_u = u * thick_u
            if not last:
                flux_u = jnp.concatenate([jnp.where(given, u[:, :cols], flux_u[:, :cols]), flux_u[:, cols:]], axis=1)
            flux_v = v * thick_v
            new = h - FLUX_STEP * (flux_u - west(flux_u) + flux_v - south(flux_v))
            if last:
                out_h[k] = new[:rows, :cols]
            else:
                deep[k] = new
            deep[layers + k] = trial_u
            deep[2 * layers + k] = trial_v
            return press_u, press_v, total_u + thick_u * trial_u, total_v + thick_v * trial_v

        zero = jnp.zeros((short, cols + LANES), jnp.float32)
        _, _, total_u, total_v = lax.fori_loop(0, layers, first_pass, (zero, zero, zero, zero))
        fix_u = (shared[4 + 2 * step] - total_u) * shared[0]
        fix_v = (shared[5 + 2 * step] - total_v) * shared[1]

        def second_pass(k, carry):
            new_u = shared[2] * (deep[layers + k] + fix_u)
            new_v = shared[3] * (deep[2 * layers + k] + fix_v)
            if last:
                out_u[k] = new_u[:rows, :cols]
                out_v[k] = new_v[:rows, :cols]
            else:
                deep[layers + k] = new_u
                deep[2 * layers + k] = new_v
            return carry

        lax.fori_loop(0, layers, second_pass, 0)


def advance_kernel(
    merid, fields, thick, vu, vv, east_in, west_in, north_in, south_in, fold_in,
    out_eta, out_bu, out_bv, out_h, out_u, out_v, shared, wide, deep,
):
    layers = thick.shape[0]
    start = FIELDS * HALO
    wide_kernel(
        merid, layers, fields, east_in, west_in, north_in, south_in, fold_in, out_eta, out_bu, out_bv, shared, wide
    )
    layers_kernel(
        merid, thick, vu, vv, east_in.at[pl.ds(start, 3 * layers)], west_in.at[pl.ds(start, 4 * layers)],
        north_in, south_in, fold_in, shared, out_h, out_u, out_v, deep,
    )


def body(
    height,
    transport_u,
    transport_v,
    thickness,
    velocity_u,
    velocity_v,
    sea_faces,
    wind_seeds,
    wind_scale,
    wind_base,
):
    layers, rows, cols = thickness.shape
    f32 = jnp.float32
    zonal = lax.axis_size("zonal")
    merid = lax.axis_size("merid")
    tall = rows + 2 * HALO
    short = rows + EDGE

    def shape(*dims):
        return jax.ShapeDtypeStruct(dims, f32)

    fields, wide_west, wide_east, packs, strips_west, strips_east = pl.pallas_call(
        lambda *refs: prepare_kernel(rows * zonal, cols * merid, *refs),
        out_shape=(
            shape(FIELDS, rows, cols),
            shape(FIELDS * HALO + 3 * layers, cols),
            shape(FIELDS * HALO + 4 * layers, cols),
            shape(4, rows, LANES),
            shape(2 * HALO + EDGE, LANES),
            shape(2 * HALO + EDGE, LANES),
        ),
        in_specs=[SMEM, SMEM] + [VMEM] * 8,
        out_specs=(VMEM,) * 6,
        name="prepare",
    )(wind_seeds.T, wind_scale, height, transport_u, transport_v, thickness, velocity_u, velocity_v, sea_faces, wind_base)

    up = [(i, (i + 1) % zonal) for i in range(zonal)]
    down = [(j, i) for i, j in up]
    strips_from_east = lax.ppermute(strips_west, "zonal", down)
    strips_from_west = lax.ppermute(strips_east, "zonal", up)
    wide_from_east = lax.ppermute(wide_west, "zonal", down)
    wide_from_west = lax.ppermute(wide_east, "zonal", up)

    swap, high, fold = pl.pallas_call(
        lambda *refs: pack_kernel(merid, *refs),
        out_shape=(shape(tall + short, LANES),) * 3,
        in_specs=[VMEM] * 3,
        out_specs=(VMEM,) * 3,
        name="pack",
    )(packs, strips_from_east, strips_from_west)

    mirror = [(i * merid + merid - 1, (zonal - 1 - i) * merid + merid - 1) for i in range(zonal)]
    folded = lax.ppermute(fold, ("zonal", "merid"), mirror)
    if merid == 2:
        from_north = lax.ppermute(swap, "merid", [(0, 1), (1, 0)])
        from_south = from_north
    else:
        from_north = lax.ppermute(swap, "merid", [(i + 1, i) for i in range(merid - 1)])
        from_south = lax.ppermute(high, "merid", [(i, i + 1) for i in range(merid - 1)])

    flat = shape(rows, cols)
    full = shape(layers, rows, cols)
    return pl.pallas_call(
        lambda *refs: advance_kernel(merid, *refs),
        out_shape=(flat, flat, flat, full, full, full),
        in_specs=[VMEM] * 9,
        out_specs=(VMEM,) * 6,
        scratch_shapes=[
            pltpu.VMEM((4 + 2 * STEPS, short, cols + LANES), f32),
            pltpu.VMEM((FIELDS, tall, cols + LANES), f32),
            pltpu.VMEM((3 * layers, short, cols + LANES), f32),
        ],
        name="advance",
    )(fields, thickness, velocity_u, velocity_v, wide_from_east, wide_from_west, from_north, from_south, folded)


def solution(mesh):
    placed = (
        P(("members", "zonal"), "merid"),
        P(("members", "zonal"), "merid"),
        P(("members", "zonal"), "merid"),
        P(None, ("members", "zonal"), "merid"),
        P(None, ("members", "zonal"), "merid"),
        P(None, ("members", "zonal"), "merid"),
        P(None, "zonal", "merid"),
        P("members", None),
        P("members"),
        P(None, "zonal", "merid"),
    )

    return jax.shard_map(
        body,
        mesh=mesh,
        in_specs=placed,
        out_specs=(
            P(("members", "zonal"), "merid"),
            P(("members", "zonal"), "merid"),
            P(("members", "zonal"), "merid"),
            P(None, ("members", "zonal"), "merid"),
            P(None, ("members", "zonal"), "merid"),
            P(None, ("members", "zonal"), "merid"),
        ),
        check_vma=False,
    )
```

```python
import math

import jax
import jax.numpy as jnp
from jax import lax
from jax.experimental import pallas as pl
from jax.experimental.pallas import tpu as pltpu
from jax.sharding import PartitionSpec as P


NSUB = 6
STEPS = 2
WAVE_LIMIT = 0.225
STRESS_SCALE = 0.1
FLUX_STEP = 0.05
PRESS_COEF = 0.05

FIELDS = 8
HALO = NSUB * STEPS
SLOT = 16
LANES = 128
EDGE = 8

VMEM = pl.BlockSpec(memory_space=pltpu.VMEM)
SMEM = pl.BlockSpec(memory_space=pltpu.SMEM)


def whole_mod(product, total):
    rest = product - jnp.floor(product * (1.0 / total)) * total
    rest = jnp.where(rest < 0.0, rest + total, rest)
    return jnp.where(rest >= total, rest - total, rest)


def prepare_kernel(
    total_x, total_y, seeds, scale, eta, bu, bv, thick, vu, vv, faces, base,
    fields, to_west, to_east, packs, strips_west, strips_east,
):
    layers, rows, cols = thick.shape
    modes = scale.shape[0]
    f32 = jnp.float32

    lane = lax.broadcasted_iota(jnp.int32, (rows, LANES), 1)
    sub = lax.broadcasted_iota(jnp.int32, (8, cols), 0)
    wave_x = jnp.zeros((rows, LANES), f32)
    wave_y = jnp.zeros((8, cols), f32)
    for m in range(modes):
        wave_x = jnp.where(lane == m, seeds[0, m].astype(f32), wave_x)
        wave_y = jnp.where(sub == m, seeds[1, m].astype(f32), wave_y)
    col = (lax.broadcasted_iota(jnp.int32, (rows, LANES), 0) + lax.axis_index("zonal") * rows).astype(f32)
    row = (lax.broadcasted_iota(jnp.int32, (8, cols), 1) + lax.axis_index("merid") * cols).astype(f32)
    angle_x = whole_mod(wave_x * col, total_x) * (2.0 * math.pi / total_x)
    angle_y = whole_mod(wave_y * row, total_y) * (2.0 * math.pi / total_y)
    cos_x, sin_x = jnp.cos(angle_x), jnp.sin(angle_x)
    cos_y, sin_y = jnp.cos(angle_y), jnp.sin(angle_y)
    sum_cos = base[0]
    sum_sin = base[1]
    for m in range(modes):
        amp = scale[m]
        ca = cos_x[:, m : m + 1] * amp
        sa = sin_x[:, m : m + 1] * amp
        cb = cos_y[m : m + 1, :]
        sb = sin_y[m : m + 1, :]
        sum_cos = sum_cos + (ca * cb - sa * sb)
        sum_sin = sum_sin + (sa * cb + ca * sb)
    fields[0] = eta[...]
    fields[1] = bu[...]
    fields[2] = bv[...]
    total = thick[0]
    for k in range(1, layers):
        total = total + thick[k]
    fields[3] = total
    fields[4] = faces[0].astype(f32)
    fields[5] = faces[1].astype(f32)
    fields[6] = STRESS_SCALE * sum_cos
    fields[7] = STRESS_SCALE * sum_sin
    for f in range(FIELDS):
        value = fields[f]
        to_west[f * HALO : (f + 1) * HALO, :] = value[:HALO]
        to_east[f * HALO : (f + 1) * HALO, :] = value[rows - HALO :]
    start = FIELDS * HALO
    edge_rows(thick, vu, vv, to_west.at[pl.ds(start, 3 * layers)], to_east.at[pl.ds(start, 4 * layers)])
    for side, low in enumerate((True, False)):
        tile = slice(0, LANES) if low else slice(cols - LANES, cols)
        acc = jnp.zeros((rows, LANES), f32)
        for f in range(FIELDS):
            moved = pltpu.roll(fields[f, :, tile], (f * SLOT + (0 if low else SLOT)) % LANES, 1)
            acc = jnp.where(lane // SLOT == f, moved, acc)
        deep = jnp.zeros((rows, LANES), f32)
        for s, own in enumerate((thick, vu, vv)):
            for k in range(layers):
                at = 2 * (s * layers + k)
                moved = pltpu.roll(own[k, :, tile], (at + (0 if low else 2)) % LANES, 1)
                deep = jnp.where(lane // 2 == s * layers + k, moved, deep)
        packs[2 * side] = acc
        packs[2 * side + 1] = deep
    for side in range(2):
        acc = packs[2 * side]
        strips_west[side * HALO : (side + 1) * HALO, :] = acc[:HALO]
        strips_east[side * HALO : (side + 1) * HALO, :] = acc[rows - HALO :]
        deep = packs[2 * side + 1]
        strips_west[2 * HALO + side : 2 * HALO + side + 1, :] = deep[:1]
        strips_east[2 * HALO + side : 2 * HALO + side + 1, :] = deep[rows - 1 :]
    used = 2 * HALO + 2
    strips_west[used:, :] = jnp.zeros((strips_west.shape[0] - used, LANES), f32)
    strips_east[used:, :] = jnp.zeros((strips_east.shape[0] - used, LANES), f32)


def edge_rows(thick, vu, vv, to_west, to_east):
    layers, rows, _ = thick.shape
    n = layers
    for k in range(layers):
        to_west[k : k + 1, :] = thick[k, 0:1, :]
        to_west[n + k : n + k + 1, :] = vu[k, 0:1, :] * ((thick[k, 0:1, :] + thick[k, 1:2, :]) * 0.5)
        to_west[2 * n + k : 2 * n + k + 1, :] = vv[k, 0:1, :]
        near = thick[k, rows - 2 : rows - 1, :]
        last = thick[k, rows - 1 : rows, :]
        to_east[k : k + 1, :] = last
        to_east[n + k : n + k + 1, :] = vu[k, rows - 2 : rows - 1, :] * ((near + last) * 0.5)
        to_east[2 * n + k : 2 * n + k + 1, :] = vu[k, rows - 1 : rows, :]
        to_east[3 * n + k : 3 * n + k + 1, :] = vv[k, rows - 1 : rows, :]


def fill_fields(target, f, fields, east, west, rows):
    cols = fields.shape[-1]
    target[f, 0:rows, 0:cols] = fields[f]
    target[f, rows : rows + HALO, 0:cols] = east[f * HALO : (f + 1) * HALO, :]
    target[f, rows + HALO : rows + 2 * HALO, 0:cols] = west[f * HALO : (f + 1) * HALO, :]


def fill_layers(target, k, layers, thick, vu, vv, east, west, rows):
    cols = thick.shape[-1]
    n = layers
    e, w = rows, rows + EDGE
    zero = jnp.zeros((EDGE, cols), jnp.float32)
    for s, own in enumerate((thick, vu, vv)):
        target[s * n + k, 0:rows, 0:cols] = own[k]
        target[s * n + k, rows : rows + EDGE, 0:cols] = zero
    target[k, e : e + 1, 0:cols] = east[k : k + 1, :]
    target[k, w - 1 : w, 0:cols] = west[k : k + 1, :]
    target[n + k, e : e + 1, 0:cols] = east[n + k : n + k + 1, :]
    target[n + k, w - 2 : w - 1, 0:cols] = west[n + k : n + k + 1, :]
    target[n + k, w - 1 : w, 0:cols] = west[2 * n + k : 2 * n + k + 1, :]
    target[2 * n + k, e : e + 1, 0:cols] = east[2 * n + k : 2 * n + k + 1, :]
    target[2 * n + k, w - 1 : w, 0:cols] = west[3 * n + k : 3 * n + k + 1, :]


def flipped(pack, rows, group):
    size = pack.shape[0]
    q = lax.broadcasted_iota(jnp.int32, (size, size), 0)
    p = lax.broadcasted_iota(jnp.int32, (size, size), 1)
    source = rows - 1 - q
    source = jnp.where(source < 0, source + size, source)
    flip_rows = (p == source).astype(jnp.float32)
    a = lax.broadcasted_iota(jnp.int32, (LANES, LANES), 0)
    b = lax.broadcasted_iota(jnp.int32, (LANES, LANES), 1)
    inner = jnp.bitwise_and(b, group - 1)
    flip_lanes = (a == b - inner + (group - 1 - inner)).astype(jnp.float32)
    half = jnp.dot(flip_rows, pack, precision=lax.Precision.HIGHEST, preferred_element_type=jnp.float32)
    return jnp.dot(half, flip_lanes, precision=lax.Precision.HIGHEST, preferred_element_type=jnp.float32)


def pack_kernel(merid, packs, east, west, swap, high, fold):
    rows = packs.shape[1]
    tall = rows + 2 * HALO
    short = rows + EDGE
    at_bottom = lax.axis_index("merid") == 0
    both = []
    for side in range(2):
        acc = jnp.concatenate(
            [packs[2 * side], east[side * HALO : (side + 1) * HALO, :], west[side * HALO : (side + 1) * HALO, :]], axis=0
        )
        high[tall : tall + rows, :] = packs[2 * side + 1]
        high[tall + rows :, :] = jnp.zeros((EDGE, LANES), jnp.float32)
        row = 2 * HALO + side
        high[tall + rows : tall + rows + 1, :] = east[row : row + 1, :]
        high[tall + short - 1 : tall + short, :] = west[row : row + 1, :]
        both.append((acc, high[tall : tall + short, :]))
    (low_f, low_l), (high_f, high_l) = both
    high[0:tall, :] = high_f
    if merid == 2:
        low_f = jnp.where(at_bottom, high_f, low_f)
        low_l = jnp.where(at_bottom, high_l, low_l)
    swap[0:tall, :] = low_f
    swap[tall : tall + short, :] = low_l
    fold[0:tall, :] = flipped(high_f, rows, SLOT)
    fold[tall : tall + short, :] = flipped(high_l, rows, 2)


def make_neighbours(ghost, cols):
    def east(a):
        n = a.shape[0]
        g = ghost[n]
        plus = pltpu.roll(a, n - 1, 0)
        return jnp.concatenate(
            [plus[:, :cols], jnp.where(g, pltpu.roll(a[:, cols:], 1, 0), plus[:, cols:])], axis=1
        )

    def west(a):
        n = a.shape[0]
        g = ghost[n]
        minus = pltpu.roll(a, 1, 0)
        return jnp.concatenate(
            [minus[:, :cols], jnp.where(g, pltpu.roll(a[:, cols:], n - 1, 0), minus[:, cols:])], axis=1
        )

    def north(a):
        g = ghost[a.shape[0]]
        plus = pltpu.roll(a, cols + LANES - 1, 1)
        minus = pltpu.roll(a[:, cols - LANES :], 1, 1)[:, LANES:]
        return jnp.concatenate([plus[:, :cols], jnp.where(g, minus, plus[:, cols:])], axis=1)

    def south(a):
        g = ghost[a.shape[0]]
        minus = pltpu.roll(a, 1, 1)
        plus = pltpu.roll(a[:, cols:], LANES - 1, 1)
        return jnp.concatenate([minus[:, :cols], jnp.where(g, plus, minus[:, cols:])], axis=1)

    return east, west, north, south


def setting(merid, sizes, cols):
    m = lax.axis_index("merid")
    top = m == merid - 1
    lanes = {n: lax.broadcasted_iota(jnp.int32, (n, LANES), 1) for n in sizes}
    ghost = {n: jnp.logical_and(top, lanes[n] < LANES // 2) for n in sizes}
    return m == 0, top, lanes, make_neighbours(ghost, cols)


def wide_kernel(
    merid, layers, fields, east_in, west_in, north_in, south_in, fold_in, out_eta, out_bu, out_bv, shared, wide,
):
    _, rows, cols = fields.shape
    tall = rows + 2 * HALO
    short = rows + EDGE
    bottom, top, lanes, (east, west, north, south) = setting(merid, (tall, short), cols)

    pack_n = jnp.where(top, fold_in[0:tall, :], north_in[0:tall, :])
    pack_s = jnp.where(bottom, 0.0, south_in[0:tall, :])
    for f in range(FIELDS):
        fill_fields(wide, f, fields, east_in, west_in, rows)
        up = pltpu.roll(pack_n, (-f * SLOT) % LANES, 1)
        down = pltpu.roll(pack_s, (LANES - SLOT - f * SLOT) % LANES, 1)
        edge = jnp.where(lanes[tall] >= LANES - SLOT, down, 0.0)
        wide[f, :, cols:] = jnp.where(lanes[tall] < SLOT, up, edge)

    near = lax.broadcasted_iota(jnp.int32, (EDGE, cols + LANES), 0) < EDGE // 2

    def shorten(a):
        return jnp.concatenate([a[:rows], jnp.where(near, a[rows : rows + EDGE], a[tall - EDGE :])], axis=0)

    total = wide[3]
    total_short = shorten(total)
    depth_u = (total_short + east(total_short)) * 0.5
    depth_v = (total_short + north(total_short)) * 0.5
    shared[0] = 1.0 / jnp.where(depth_u > 0.0, depth_u, 1.0)
    shared[1] = 1.0 / jnp.where(depth_v > 0.0, depth_v, 1.0)
    shared[2] = shorten(wide[4])
    shared[3] = shorten(wide[5])
    wide[3] = (WAVE_LIMIT / layers) * total
    eta = wide[0]
    bu = wide[1]
    bv = wide[2]
    for step in range(STEPS):
        sum_u = jnp.zeros_like(bu)
        sum_v = jnp.zeros_like(bv)
        for _ in range(NSUB):
            eta = eta - (bu - west(bu) + bv - south(bv))
            bu = wide[4] * (bu - wide[3] * (east(eta) - eta) + wide[6])
            bv = wide[5] * (bv - wide[3] * (north(eta) - eta) + wide[7])
            sum_u = sum_u + bu
            sum_v = sum_v + bv
        shared[4 + 2 * step] = shorten(sum_u) * (1.0 / NSUB)
        shared[5 + 2 * step] = shorten(sum_v) * (1.0 / NSUB)
    out_eta[...] = eta[:rows, :cols]
    out_bu[...] = bu[:rows, :cols]
    out_bv[...] = bv[:rows, :cols]


def layers_kernel(
    merid, thick, vu, vv, east_in, west_in, north_in, south_in, fold_in, shared, out_h, out_u, out_v, deep,
):
    layers, rows, cols = thick.shape
    tall = rows + 2 * HALO
    short = rows + EDGE
    bottom, top, lanes, (east, west, north, south) = setting(merid, (short,), cols)
    deep_n = jnp.where(top, fold_in[tall : tall + short, :], north_in[tall : tall + short, :])
    deep_s = jnp.where(bottom, 0.0, south_in[tall : tall + short, :])
    for k in range(layers):
        fill_layers(deep, k, layers, thick, vu, vv, east_in, west_in, rows)
    for k in range(3 * layers):
        up = pltpu.roll(deep_n, (-2 * k) % LANES, 1)
        down = pltpu.roll(deep_s, (LANES - 2 - 2 * k) % LANES, 1)
        edge = jnp.where(lanes[short] >= LANES - 2, down, 0.0)
        deep[k, :, cols:] = jnp.where(lanes[short] < 2, up, edge)
    spot = lax.broadcasted_iota(jnp.int32, (EDGE, cols), 0)
    given = jnp.logical_or(spot == 0, spot == EDGE - 2)

    for step in range(STEPS):
        last = step == STEPS - 1

        def first_pass(k, carry):
            press_u, press_v, total_u, total_v = carry
            h = deep[k]
            u = deep[layers + k]
            v = deep[2 * layers + k]
            east_h = east(h)
            north_h = north(h)
            thick_u = (h + east_h) * 0.5
            thick_v = (h + north_h) * 0.5
            press_u = press_u + (east_h - h)
            press_v = press_v + (north_h - h)
            trial_u = u - PRESS_COEF * press_u
            trial_v = v - PRESS_COEF * press_v
            flux_u = u * thick_u
            if not last:
                outer = jnp.where(given, u[rows:, :cols], flux_u[rows:, :cols])
                inside = jnp.concatenate([flux_u[:rows, :cols], outer], axis=0)
                flux_u = jnp.concatenate([inside, flux_u[:, cols:]], axis=1)
            flux_v = v * thick_v
            new = h - FLUX_STEP * (flux_u - west(flux_u) + flux_v - south(flux_v))
            if last:
                out_h[k] = new[:rows, :cols]
            else:
                deep[k] = new
            deep[layers + k] = trial_u
            deep[2 * layers + k] = trial_v
            return press_u, press_v, total_u + thick_u * trial_u, total_v + thick_v * trial_v

        zero = jnp.zeros((short, cols + LANES), jnp.float32)
        _, _, total_u, total_v = lax.fori_loop(0, layers, first_pass, (zero, zero, zero, zero))
        fix_u = (shared[4 + 2 * step] - total_u) * shared[0]
        fix_v = (shared[5 + 2 * step] - total_v) * shared[1]

        def second_pass(k, carry):
            new_u = shared[2] * (deep[layers + k] + fix_u)
            new_v = shared[3] * (deep[2 * layers + k] + fix_v)
            if last:
                out_u[k] = new_u[:rows, :cols]
                out_v[k] = new_v[:rows, :cols]
            else:
                deep[layers + k] = new_u
                deep[2 * layers + k] = new_v
            return carry

        lax.fori_loop(0, layers, second_pass, 0)


def advance_kernel(
    merid, fields, thick, vu, vv, east_in, west_in, north_in, south_in, fold_in,
    out_eta, out_bu, out_bv, out_h, out_u, out_v, shared, wide, deep,
):
    layers = thick.shape[0]
    start = FIELDS * HALO
    wide_kernel(
        merid, layers, fields, east_in, west_in, north_in, south_in, fold_in, out_eta, out_bu, out_bv, shared, wide
    )
    layers_kernel(
        merid, thick, vu, vv, east_in.at[pl.ds(start, 3 * layers)], west_in.at[pl.ds(start, 4 * layers)],
        north_in, south_in, fold_in, shared, out_h, out_u, out_v, deep,
    )


def body(
    height,
    transport_u,
    transport_v,
    thickness,
    velocity_u,
    velocity_v,
    sea_faces,
    wind_seeds,
    wind_scale,
    wind_base,
):
    layers, rows, cols = thickness.shape
    f32 = jnp.float32
    zonal = lax.axis_size("zonal")
    merid = lax.axis_size("merid")
    tall = rows + 2 * HALO
    short = rows + EDGE

    def shape(*dims):
        return jax.ShapeDtypeStruct(dims, f32)

    fields, wide_west, wide_east, packs, strips_west, strips_east = pl.pallas_call(
        lambda *refs: prepare_kernel(rows * zonal, cols * merid, *refs),
        out_shape=(
            shape(FIELDS, rows, cols),
            shape(FIELDS * HALO + 3 * layers, cols),
            shape(FIELDS * HALO + 4 * layers, cols),
            shape(4, rows, LANES),
            shape(2 * HALO + EDGE, LANES),
            shape(2 * HALO + EDGE, LANES),
        ),
        in_specs=[SMEM, SMEM] + [VMEM] * 8,
        out_specs=(VMEM,) * 6,
        name="prepare",
    )(wind_seeds.T, wind_scale, height, transport_u, transport_v, thickness, velocity_u, velocity_v, sea_faces, wind_base)

    up = [(i, (i + 1) % zonal) for i in range(zonal)]
    down = [(j, i) for i, j in up]
    strips_from_east = lax.ppermute(strips_west, "zonal", down)
    strips_from_west = lax.ppermute(strips_east, "zonal", up)
    wide_from_east = lax.ppermute(wide_west, "zonal", down)
    wide_from_west = lax.ppermute(wide_east, "zonal", up)

    swap, high, fold = pl.pallas_call(
        lambda *refs: pack_kernel(merid, *refs),
        out_shape=(shape(tall + short, LANES),) * 3,
        in_specs=[VMEM] * 3,
        out_specs=(VMEM,) * 3,
        name="pack",
    )(packs, strips_from_east, strips_from_west)

    mirror = [(i * merid + merid - 1, (zonal - 1 - i) * merid + merid - 1) for i in range(zonal)]
    folded = lax.ppermute(fold, ("zonal", "merid"), mirror)
    if merid == 2:
        from_north = lax.ppermute(swap, "merid", [(0, 1), (1, 0)])
        from_south = from_north
    else:
        from_north = lax.ppermute(swap, "merid", [(i + 1, i) for i in range(merid - 1)])
        from_south = lax.ppermute(high, "merid", [(i, i + 1) for i in range(merid - 1)])

    flat = shape(rows, cols)
    full = shape(layers, rows, cols)
    return pl.pallas_call(
        lambda *refs: advance_kernel(merid, *refs),
        out_shape=(flat, flat, flat, full, full, full),
        in_specs=[VMEM] * 9,
        out_specs=(VMEM,) * 6,
        scratch_shapes=[
            pltpu.VMEM((4 + 2 * STEPS, short, cols + LANES), f32),
            pltpu.VMEM((FIELDS, tall, cols + LANES), f32),
            pltpu.VMEM((3 * layers, short, cols + LANES), f32),
        ],
        name="advance",
    )(fields, thickness, velocity_u, velocity_v, wide_from_east, wide_from_west, from_north, from_south, folded)


def solution(mesh):
    placed = (
        P(("members", "zonal"), "merid"),
        P(("members", "zonal"), "merid"),
        P(("members", "zonal"), "merid"),
        P(None, ("members", "zonal"), "merid"),
        P(None, ("members", "zonal"), "merid"),
        P(None, ("members", "zonal"), "merid"),
        P(None, "zonal", "merid"),
        P("members", None),
        P("members"),
        P(None, "zonal", "merid"),
    )

    return jax.shard_map(
        body,
        mesh=mesh,
        in_specs=placed,
        out_specs=(
            P(("members", "zonal"), "merid"),
            P(("members", "zonal"), "merid"),
            P(("members", "zonal"), "merid"),
            P(None, ("members", "zonal"), "merid"),
            P(None, ("members", "zonal"), "merid"),
            P(None, ("members", "zonal"), "merid"),
        ),
        check_vma=False,
    )
```
